512 devices in a mesh: lon: 32 (over z, core), lat: 4 (over y), lev: 4 (over x).
Axes of the slice: x: 4, y: 4, z: 16, core: 2. Of those that a mesh axis runs over, the one named last changes fastest.
Arguments:
- fields: float32 [3, 8, 960, 512], P(None, 'lev', 'lon', 'lat'), may hold values from -6 to 6
- spectral_coeffs: float32 [3, 8], P(None, 'lev'), may hold values from 0.3 to 3
- mlp_in: bfloat16 [384, 24], replicated, may hold values from -1.25 to 1.25
- mlp_mid: bfloat16 [2, 384, 384], replicated, may hold values from -0.3125 to 0.3125
- mlp_out: bfloat16 [24, 384], replicated, may hold values from -0.3125 to 0.3125
Outputs:
- updated: float32 [3, 8, 960, 512], P(None, 'lev', 'lon', 'lat')
The draws below stay inside these ranges and needn't reach their ends.
All inputs are finite; a program needn't handle non-finite values.
Results may differ from the reference program's by a relative error of at most 0.0012.
Values may be sent and summed in bfloat16 or wider, within the bound.
A program may use at most 64 MiB of HBM per device.

```python
import math
import jax
import jax.numpy as jnp
from jax import lax

WAVES = 320
KMAX = 320
UNITS = 384
SUBSTEPS = 2
NLON = 960
NLAT = 512
LEVELS = 8


def block_levels(stream_key, dims, shards, low, largest):
    factor_of, own = 1.0, jax.random.fold_in(stream_key, 6)
    for position, blocks in shards:
        steps = jnp.exp(jax.random.uniform(jax.random.fold_in(own, position), (blocks,), jnp.float32, low / len(shards), largest / len(shards)))
        factor_of = factor_of * jnp.repeat(steps, dims[position] // blocks).reshape([-1 if axis == position else 1 for axis in range(len(dims))])
    return factor_of


def bell_draw(stream_key, shape, scale, reach, pieces=(), kind=jnp.bfloat16):
    factor_of = block_levels(stream_key, shape, pieces, -0.22, 0.18) if pieces else 1.0
    array = jax.random.normal(stream_key, shape, jnp.float32) * scale * factor_of
    return jnp.minimum(jnp.maximum(array, -reach), reach).astype(kind)


def setup_inputs(seed: int = 0) -> dict:
    key_of = jax.random.split(jax.random.key(seed), 6)
    return {
        "fields": bell_draw(key_of[0], (3, LEVELS, NLON, NLAT), 1.0, 6.0, ((1, 4), (2, 32), (3, 4)), jnp.float32),
        "spectral_coeffs": jnp.clip(jnp.exp(math.log(3.0) - 2.3025851 * jax.random.uniform(key_of[1], (3, LEVELS), jnp.float32) ** block_levels(key_of[1], (3, LEVELS), ((1, 4),), -0.2, 0.2)), 0.3, 3.0),
        "mlp_in": bell_draw(key_of[2], (UNITS, 3 * LEVELS), (3 * LEVELS) ** -0.5, 1.25),
        "mlp_mid": bell_draw(key_of[3], (2, UNITS, UNITS), UNITS ** -0.5, 0.3125),
        "mlp_out": bell_draw(key_of[4], (3 * LEVELS, UNITS), UNITS ** -0.5, 0.3125),
    }


highest = lax.Precision.HIGHEST


def forward_table(lon_ids, total_lon, waves):
    wave_ids = jnp.arange(waves, dtype=jnp.int32)
    phase = ((lon_ids[:, None] * wave_ids[None, :]) % total_lon).astype(jnp.float32) * (2.0 * jnp.pi / total_lon)
    return jnp.concatenate([jnp.cos(phase), -jnp.sin(phase)], axis=1) / total_lon


def inverse_table(lon_ids, total_lon, waves):
    wave_ids = jnp.arange(waves, dtype=jnp.int32)
    phase = ((wave_ids[:, None] * lon_ids[None, :]) % total_lon).astype(jnp.float32) * (2.0 * jnp.pi / total_lon)
    weight = jnp.where(wave_ids == 0, 1.0, 2.0).astype(jnp.float32)[:, None]
    return jnp.concatenate([weight * jnp.cos(phase), -weight * jnp.sin(phase)], axis=0)


def latitude_tables(lat_ids, total_lat, degree_ids):
    odd_rows = 2 * lat_ids[:, None] + 1
    period = 4 * total_lat
    scale = jnp.pi / (2.0 * total_lat)
    even_arg = ((odd_rows * degree_ids[None, :]) % period).astype(jnp.float32) * scale
    odd_arg = ((odd_rows * (degree_ids[None, :] + 1)) % period).astype(jnp.float32) * scale
    return jnp.cos(even_arg), jnp.sin(odd_arg)


def latitude_forward(waves, even_tab, odd_tab):
    cols, nf, levs, lats = waves.shape
    pairs = waves.reshape(cols // 2, 2, nf, levs, lats)
    even_part = jnp.einsum("pfli,ik->pflk", pairs[:, 0], even_tab, precision=highest)
    odd_part = jnp.einsum("pfli,ik->pflk", pairs[:, 1], odd_tab, precision=highest)
    return jnp.stack([even_part, odd_part], axis=1).reshape(cols, nf, levs, even_tab.shape[1])


def latitude_inverse(spectra, even_tab, odd_tab):
    cols, nf, levs, degs = spectra.shape
    pairs = spectra.reshape(cols // 2, 2, nf, levs, degs)
    even_part = jnp.einsum("pflk,ik->pfli", pairs[:, 0], even_tab, precision=highest)
    odd_part = jnp.einsum("pflk,ik->pfli", pairs[:, 1], odd_tab, precision=highest)
    return jnp.stack([even_part, odd_part], axis=1).reshape(cols, nf, levs, even_tab.shape[0])


def operator(spectra, coeffs, col_waves, degree_ids):
    parity = col_waves % 2
    freq = (degree_ids[None, :] + parity[:, None]).astype(jnp.float32)
    wavenum = col_waves.astype(jnp.float32)[:, None]
    qvalue = ((wavenum * wavenum + freq * freq) / (KMAX * KMAX))[:, None, :]
    hyper = coeffs[0][None, :, None]
    coupling = coeffs[1][None, :, None]
    depth = coeffs[2][None, :, None]
    vort = spectra[:, 0]
    diverg = spectra[:, 1]
    temper = spectra[:, 2]
    new_vort = vort / (1.0 + hyper * qvalue * qvalue)
    new_div = (diverg + coupling * qvalue * temper) / (1.0 + coupling * depth * qvalue)
    new_temp = temper - depth * new_div
    return jnp.stack([new_vort - vort, new_div - diverg, new_temp - temper], axis=1)


def nonlinear(state):
    temper = state[2] + 0.25 * state[0] * state[1]
    return jnp.stack([state[0], state[1], temper], axis=0)


def reference(fields, spectral_coeffs, mlp_in, mlp_mid, mlp_out):
    nf, levels, total_lon, total_lat = fields.shape
    lon_ids = jnp.arange(total_lon, dtype=jnp.int32)
    fwd_tab = forward_table(lon_ids, total_lon, WAVES)
    inv_tab = inverse_table(lon_ids, total_lon, WAVES)
    even_tab, odd_tab = latitude_tables(jnp.arange(total_lat, dtype=jnp.int32), total_lat, jnp.arange(KMAX, dtype=jnp.int32))
    weight = 2.0 / total_lat
    col_waves = jnp.arange(2 * WAVES, dtype=jnp.int32) % WAVES
    degree_ids = jnp.arange(KMAX, dtype=jnp.int32)
    state = fields
    for substep in range(SUBSTEPS):
        waves = jnp.einsum("flji,jc->cfli", state, fwd_tab, precision=highest)
        spectra = latitude_forward(waves, even_tab * weight, odd_tab * weight)
        change = operator(spectra, spectral_coeffs, col_waves, degree_ids)
        back = latitude_inverse(change, even_tab, odd_tab)
        increment = jnp.einsum("cfli,cj->flji", back, inv_tab, precision=highest)
        state = nonlinear(state + increment)

    def column_block(block):
        inputs = block.astype(jnp.bfloat16).reshape(nf * levels, total_lat)
        hidden = jax.nn.silu(jnp.dot(mlp_in, inputs, preferred_element_type=jnp.float32)).astype(jnp.bfloat16)
        hidden = jax.nn.silu(jnp.dot(mlp_mid[0], hidden, preferred_element_type=jnp.float32)).astype(jnp.bfloat16)
        hidden = jax.nn.silu(jnp.dot(mlp_mid[1], hidden, preferred_element_type=jnp.float32)).astype(jnp.bfloat16)
        output = jnp.dot(mlp_out, hidden, preferred_element_type=jnp.float32).astype(jnp.bfloat16)
        return output.reshape(nf, levels, total_lat)

    correction = lax.map(column_block, state.transpose(2, 0, 1, 3)).transpose(1, 2, 0, 3)
    return state + correction.astype(jnp.float32)
```

```python
import functools

import jax
import jax.numpy as jnp
import numpy as np
from jax import lax
from jax.experimental import pallas as pl
from jax.experimental.pallas import tpu as pltpu
from jax.sharding import PartitionSpec as P

WAVES = 320
KMAX = 320
SUBSTEPS = 2
NLON = 960
NLAT = 512
LEVELS = 8
UNITS = 384
GROUP = 64
F32 = jnp.float32
BF16 = jnp.bfloat16


def split_host(table):
    high = table.astype(np.float32).astype(BF16)
    low = (table - high.astype(np.float64)).astype(np.float32).astype(BF16)
    return np.stack([high, low])


@functools.lru_cache(None)
def host_tables():
    q = np.repeat(np.arange(10), GROUP)
    o = np.tile(np.arange(GROUP), 10)
    wave = 2 * (5 * (o // 2) + q % 5) + o % 2
    lane = np.arange(1024)
    lon = 30 * (lane // 32) + lane % 32
    phase = (wave[:, None] * lon[None, :]) % NLON * (2.0 * np.pi / NLON)
    zonal = np.where(q[:, None] < 5, np.cos(phase), -np.sin(phase)) * (lane % 32 < 30)[None, :]
    pos = np.arange(NLAT)
    lat = 8 * (pos % 64) + pos // 64
    deg = np.arange(KMAX)
    odd = 2 * lat + 1
    even = np.cos((deg[:, None] * odd[None, :]) % (4 * NLAT) * (np.pi / (2 * NLAT)))
    sine = np.sin(((deg[:, None] + 1) * odd[None, :]) % (4 * NLAT) * (np.pi / (2 * NLAT)))
    fwd = np.stack([split_host(even), split_host(sine)])
    inv = np.stack([split_host(even.T), split_host(sine.T)])
    perm = np.zeros((10, 24, 256), np.float32)
    for f in range(3):
        for i8 in range(8):
            for c in range(10):
                perm[c, f * 8 + i8, i8 * 32 + f * 10 + c] = 1.0
    gather = np.concatenate([perm, perm], axis=1).reshape(480, 256).astype(BF16)
    scatter = perm.reshape(240, 256).astype(BF16)
    return split_host(zonal), fwd, inv, gather, scatter


def split(value):
    high = value.astype(BF16)
    return high, (value - high.astype(F32)).astype(BF16)


def mm(a, b):
    return lax.dot_general(a, b, (((1,), (0,)), ((), ())), preferred_element_type=F32)


def mm_nt(a, b):
    return lax.dot_general(a, b, (((1,), (1,)), ((), ())), preferred_element_type=F32)


def silu(v):
    return 0.5 * v * (1.0 + jnp.tanh(0.5 * v))


def kernel(
    coef_ref, fields_hbm, zonal_hbm, fwd_hbm, inv_hbm, gather_hbm, scatter_hbm, w_in_hbm, w_mid_hbm, w_out_hbm,
    out_ref,
    fields, zonal, fwd, inv, gather, scatter, w_in, w_mid, w_out,
    stage, at, ra, state, vb, ub, mult, mb, rm, cr, fb, ob,
    load_sems, send_sems, recv_sems,
):
    zc = lax.axis_index("lon")
    y = lax.axis_index("lat")
    x = lax.axis_index("lev")
    z, c = lax.div(zc, 2), lax.rem(zc, 2)
    p, zb = lax.div(z, 2), lax.rem(z, 2)
    mine = x * 4 + zb * 2 + c
    me = y * 16 + mine
    own_x, own_b = lax.rem(p, 4), lax.div(p, 4)

    loads = []

    def load(n, src, dst):
        copy = pltpu.make_async_copy(src, dst, load_sems.at[n])
        copy.start()
        loads.append(copy)

    load(0, fields_hbm, fields)
    load(1, zonal_hbm, zonal)
    load(2, fwd_hbm.at[c], fwd)
    load(3, inv_hbm.at[c], inv)
    load(4, gather_hbm, gather)
    load(5, scatter_hbm, scatter)
    load(6, w_in_hbm, w_in)
    load(7, w_mid_hbm, w_mid)
    load(8, w_out_hbm, w_out)

    def group_device(g):
        return {"lon": 4 * p + lax.rem(g, 4), "lat": lax.div(g, 16), "lev": lax.div(lax.rem(g, 16), 4)}

    def first_target(t):
        b, k = lax.div(t, 16), lax.rem(t, 16)
        return {"lon": 4 * (x + 4 * b) + lax.rem(k, 4), "lat": y, "lev": lax.div(k, 4)}

    own_first = x == own_x
    self_t = own_b * 16 + mine

    barrier = pltpu.get_barrier_semaphore()

    def greet_first(j, carry):
        d = lax.rem(zc + j, 32)

        @pl.when(jnp.logical_or(d != zc, jnp.logical_not(own_first)))
        def _():
            pl.semaphore_signal(barrier, inc=1, device_id={"lon": d, "lat": y, "lev": own_x})
        return carry

    def greet_group(j, carry):
        pl.semaphore_signal(barrier, inc=1, device_id=group_device(lax.rem(me + j, GROUP)))
        return carry

    def greet_planes(j, carry):
        pl.semaphore_signal(barrier, inc=1, device_id={"lon": 2 * lax.rem(z + j, 16) + c, "lat": y, "lev": x})
        return carry

    lax.fori_loop(0, 32, greet_first, 0)
    lax.fori_loop(1, GROUP, greet_group, 0)
    lax.fori_loop(1, 16, greet_planes, 0)

    loads[0].wait()
    for b in range(2):
        for f in range(3):
            stage[32 * f : 32 * f + 30, :] = fields[f, b]
            stage[32 * f + 30 : 32 * f + 32, :] = jnp.zeros((2, 128), F32)
        for n in range(3):
            stage[96 + n : 97 + n, :] = jnp.full((1, 128), coef_ref[n, b], F32)
        stage[99:128, :] = jnp.zeros((29, 128), F32)
        at[128 * b : 128 * b + 128, :] = stage[...].T

    pl.semaphore_wait(barrier, 31 + jnp.where(own_first, 0, 1) + (GROUP - 1) + 15)

    def send_first(j, carry):
        t = lax.rem(self_t + j, 32)

        @pl.when(jnp.logical_or(j > 0, jnp.logical_not(own_first)))
        def _():
            pltpu.make_async_remote_copy(
                at.at[pl.ds(pl.multiple_of(8 * t, 8), 8), :],
                ra.at[pl.ds(pl.multiple_of(8 * zc, 8), 8), :],
                send_sems.at[0], recv_sems.at[0], device_id=first_target(t),
            ).start()
        return carry

    lax.fori_loop(0, 32, send_first, 0)

    @pl.when(own_first)
    def _():
        ra[pl.ds(pl.multiple_of(8 * zc, 8), 8), :] = at[pl.ds(pl.multiple_of(8 * self_t, 8), 8), :]

    def drain(ref, sem):
        pltpu.make_async_copy(ref, ref, sem).wait()

    for n in range(1, 9):
        loads[n].wait()

    @pl.when(own_first)
    def _():
        drain(ra.at[pl.ds(0, 248), :], recv_sems.at[0])

    @pl.when(jnp.logical_not(own_first))
    def _():
        drain(ra, recv_sems.at[0])

    lane = lax.broadcasted_iota(jnp.int32, (8, 128), 1)
    for v in range(8):
        tiles = [ra[8 * (4 * v + n) : 8 * (4 * v + n) + 8, :] for n in range(4)]
        for f in range(3):
            value = pltpu.roll(tiles[0], (-32 * f) % 128, 1)
            for n in range(1, 4):
                value = jnp.where(lane >= 32 * n, pltpu.roll(tiles[n], (32 * (n - f)) % 128, 1), value)
            state[8 * f : 8 * f + 8, 128 * v : 128 * v + 128] = value

    coefs = ra[0:1, :]

    def operator_tables():
        nu, ga, gb = coefs[:, 96:97], coefs[:, 97:98], coefs[:, 98:99]
        deg = lax.broadcasted_iota(jnp.int32, (KMAX, 32), 0)
        col = lax.broadcasted_iota(jnp.int32, (KMAX, 32), 1)
        field = jnp.where(col >= 20, 2, jnp.where(col >= 10, 1, 0))
        place = col - 10 * field
        turn = jnp.where(place >= 5, place - 5, place)
        wave = 2 * (5 * lax.div(me, 2) + turn) + c
        freq = (deg + c).astype(F32)
        wavef = wave.astype(F32)
        qv = (wavef * wavef + freq * freq) / (KMAX * KMAX)
        scale = jnp.where(wave == 0, 1.0, 2.0) * (2.0 / NLAT / NLON)
        damp = nu * qv * qv
        couple = ga * gb * qv
        den = 1.0 + jnp.where(field == 0, damp, couple)
        own = -jnp.where(field == 0, damp, couple)
        other = jnp.where(field == 0, 0.0, jnp.where(field == 1, ga * qv, -gb))
        valid = col < 30
        factor = jnp.where(valid, scale / den, 0.0)
        mult[0] = own * factor
        mult[1] = other * factor

    for step in range(SUBSTEPS):
        b_in, c_in = 2 * step, 2 * step + 1

        high, low = split(state[...])
        both = jnp.concatenate([high.astype(F32), low.astype(F32)], axis=0).astype(BF16)
        first = jnp.concatenate([high.astype(F32), jnp.zeros((24, 1024), F32)], axis=0).astype(BF16)
        value = mm_nt(zonal[0], both) + mm_nt(zonal[1], first)
        w_high, w_low = split(value)
        packed = jnp.zeros((GROUP, 256), F32)
        for q in range(10):
            rows = slice(GROUP * q, GROUP * q + GROUP)
            place = gather[48 * q : 48 * q + 48, :]
            packed = packed + mm(w_high[rows], place) + mm(w_low[rows], place)

        def exchange(n, value):
            vb[n, pl.ds(0, GROUP, stride=2), :] = value[:, :128]
            vb[n, pl.ds(1, GROUP, stride=2), :] = value[:, 128:]

            def send(j, carry):
                g = lax.rem(me + j, GROUP)
                pltpu.make_async_remote_copy(
                    vb.at[n, pl.ds(2 * g, 2), :], ub.at[n, pl.ds(2 * me, 2), :],
                    send_sems.at[1 + n], recv_sems.at[1 + n], device_id=group_device(g),
                ).start()
                return carry

            lax.fori_loop(1, GROUP, send, 0, unroll=True)
            ub[n, pl.ds(2 * me, 2), :] = vb[n, pl.ds(2 * me, 2), :]

        def received(n):
            drain(ub.at[n, pl.ds(0, 2 * GROUP - 2), :], recv_sems.at[1 + n])
            return jnp.concatenate(
                [ub[n, pl.ds(0, GROUP, stride=2), :], ub[n, pl.ds(1, GROUP, stride=2), :]], axis=1
            )

        exchange(b_in, packed)
        if step == 0:
            operator_tables()
        value = received(b_in)

        value = jnp.concatenate([value[:, 32 * n : 32 * n + 32] for n in range(8)], axis=0)
        high, low = split(value)
        spectra = mm(fwd[0], high) + mm(fwd[0], low) + mm(fwd[1], high)
        col = lax.broadcasted_iota(jnp.int32, (KMAX, 32), 1)
        up = jnp.concatenate([spectra[:, 10:], spectra[:, :10]], axis=1)
        down = jnp.concatenate([spectra[:, 22:], spectra[:, :22]], axis=1)
        change = spectra * mult[0] + jnp.where(col < 20, up, down) * mult[1]
        high, low = split(change)
        value = mm(inv[0], high) + mm(inv[0], low) + mm(inv[1], high)
        value = jnp.concatenate([value[64 * n : 64 * n + 64] for n in range(8)], axis=1)

        exchange(c_in, value)
        value = received(c_in)

        high, low = split(value)
        y_high = mm_nt(scatter[...], high)
        y_low = mm_nt(scatter[...], low)
        y_high = jnp.concatenate([y_high[24 * q : 24 * q + 24] for q in range(10)], axis=1)
        y_low = jnp.concatenate([y_low[24 * q : 24 * q + 24] for q in range(10)], axis=1)
        both = jnp.concatenate([y_high, y_low], axis=0).astype(BF16)
        value = mm(both, zonal[0])
        new = state[...] + value[:24] + value[24:] + mm(y_high.astype(BF16), zonal[1])
        state[0:16, :] = new[0:16]
        state[16:24, :] = new[16:24] + 0.25 * new[0:8] * new[8:16]

    half = lane < 64
    for t in range(16):
        v = t // 2
        s = [state[8 * f : 8 * f + 8, 128 * v : 128 * v + 128] for f in range(3)]
        if t % 2 == 0:
            mb[16 * t : 16 * t + 8, :] = jnp.where(half, s[0], pltpu.roll(s[1], 64, 1))
            mb[16 * t + 8 : 16 * t + 16, :] = s[2]
        else:
            mb[16 * t : 16 * t + 8, :] = jnp.where(half, pltpu.roll(s[0], 64, 1), s[1])
            mb[16 * t + 8 : 16 * t + 16, :] = pltpu.roll(s[2], 64, 1)
    slot = zb * 8 + 2 * own_x + own_b

    def send_planes(j, carry):
        t = lax.rem(z + j, 16)
        pltpu.make_async_remote_copy(
            mb.at[pl.ds(pl.multiple_of(16 * t, 16), 16), :], rm.at[pl.ds(pl.multiple_of(16 * slot, 16), 16), :],
            send_sems.at[5], recv_sems.at[5], device_id={"lon": 2 * t + c, "lat": y, "lev": x},
        ).start()
        return carry

    lax.fori_loop(1, 16, send_planes, 0)
    rm[pl.ds(pl.multiple_of(16 * slot, 16), 16), :] = mb[pl.ds(pl.multiple_of(16 * z, 16), 16), :]
    drain(rm.at[pl.ds(0, 240), :], recv_sems.at[5])

    for block in range(4):
        parts = []
        for i8 in (2 * block, 2 * block + 1):
            t00 = rm[pl.ds(i8, 8, stride=16), :]
            t01 = rm[pl.ds(8 + i8, 8, stride=16), :]
            t10 = rm[pl.ds(128 + i8, 8, stride=16), :]
            t11 = rm[pl.ds(128 + 8 + i8, 8, stride=16), :]
            parts.append(jnp.concatenate([
                jnp.where(half, t00, pltpu.roll(t10, 64, 1)),
                jnp.where(half, pltpu.roll(t00, 64, 1), t10),
                jnp.where(half, t01, pltpu.roll(t11, 64, 1)),
            ], axis=0))
        inputs = jnp.concatenate(parts, axis=1).astype(BF16)
        hidden = silu(mm(w_in[...], inputs)).astype(BF16)
        hidden = silu(mm(w_mid[0], hidden)).astype(BF16)
        hidden = silu(mm(w_mid[1], hidden)).astype(BF16)
        result = mm(w_out[...], hidden).astype(BF16).astype(F32)
        for n in range(2):
            for f in range(3):
                row = (f * 8 + 2 * block + n) * 8
                cr[row : row + 8, :] = result[8 * f : 8 * f + 8, 128 * n : 128 * n + 128]

    for l in range(LEVELS):
        t00 = rm[16 * l : 16 * l + 8, :]
        t01 = rm[16 * l + 8 : 16 * l + 16, :]
        t10 = rm[128 + 16 * l : 128 + 16 * l + 8, :]
        t11 = rm[128 + 16 * l + 8 : 128 + 16 * l + 16, :]
        s = [
            jnp.where(half, t00, pltpu.roll(t10, 64, 1)),
            jnp.where(half, pltpu.roll(t00, 64, 1), t10),
            jnp.where(half, t01, pltpu.roll(t11, 64, 1)),
        ]
        s = [s[f] + cr[pl.ds(64 * f + l, 8, stride=8), :] for f in range(3)]
        for bit in range(2):
            for core in range(2):
                n = 2 * bit + core
                value = pltpu.roll(s[0], (-32 * n) % 128, 1)
                for f in range(1, 3):
                    value = jnp.where(lane >= 32 * f, pltpu.roll(s[f], (32 * (f - n)) % 128, 1), value)
                row = (2 * (l // 2) + core) * 32 + (2 * (l % 2) + bit) * 8
                fb[row : row + 8, :] = value

    place = 2 * x + c

    def send_levels(j, carry):
        t = lax.rem(place + j, 8)
        pltpu.make_async_remote_copy(
            fb.at[pl.ds(pl.multiple_of(32 * t, 32), 32), :], ob.at[pl.ds(pl.multiple_of(32 * place, 32), 32), :],
            send_sems.at[6], recv_sems.at[6],
            device_id={"lon": 2 * z + lax.rem(t, 2), "lat": y, "lev": lax.div(t, 2)},
        ).start()
        return carry

    lax.fori_loop(1, 8, send_levels, 0)
    ob[pl.ds(pl.multiple_of(32 * place, 32), 32), :] = fb[pl.ds(pl.multiple_of(32 * place, 32), 32), :]
    drain(ob.at[pl.ds(0, 224), :], recv_sems.at[6])
    for b in range(2):
        rows = []
        for k in range(16):
            row = (2 * (k // 4) + k % 2) * 32 + (2 * b + (k // 2) % 2) * 8
            rows.append(ob[row : row + 8, :])
        stage[...] = jnp.concatenate(rows, axis=0).T
        for f in range(3):
            out_ref[f, b] = stage[32 * f : 32 * f + 30, :]

    @pl.when(own_first)
    def _():
        drain(at.at[pl.ds(0, 248), :], send_sems.at[0])

    @pl.when(jnp.logical_not(own_first))
    def _():
        drain(at, send_sems.at[0])

    for n in range(4):
        drain(vb.at[n, pl.ds(0, 2 * GROUP - 2), :], send_sems.at[1 + n])
    drain(mb.at[pl.ds(0, 240), :], send_sems.at[5])
    drain(fb.at[pl.ds(0, 224), :], send_sems.at[6])


def per_device(fields, spectral_coeffs, mlp_in, mlp_mid, mlp_out):
    zonal, fwd, inv, gather, scatter = (jnp.asarray(t) for t in host_tables())
    anywhere = pl.BlockSpec(memory_space=pl.ANY)
    vmem = lambda *shape: pltpu.VMEM(shape, F32)
    return pl.pallas_call(
        kernel,
        out_shape=jax.ShapeDtypeStruct(fields.shape, F32),
        in_specs=[pl.BlockSpec(memory_space=pltpu.SMEM)] + [anywhere] * 9,
        out_specs=pl.BlockSpec(memory_space=pltpu.VMEM),
        scratch_shapes=[
            pltpu.VMEM(fields.shape, F32),
            pltpu.VMEM(zonal.shape, BF16),
            pltpu.VMEM(fwd.shape[1:], BF16),
            pltpu.VMEM(inv.shape[1:], BF16),
            pltpu.VMEM(gather.shape, BF16),
            pltpu.VMEM(scatter.shape, BF16),
            pltpu.VMEM(mlp_in.shape, BF16),
            pltpu.VMEM(mlp_mid.shape, BF16),
            pltpu.VMEM(mlp_out.shape, BF16),
            vmem(128, 128),
            vmem(256, 128),
            vmem(256, 128),
            vmem(24, 1024),
            vmem(4, 128, 128),
            vmem(4, 128, 128),
            vmem(2, KMAX, 32),
            vmem(256, 128),
            vmem(256, 128),
            vmem(192, 128),
            vmem(256, 128),
            vmem(256, 128),
            pltpu.SemaphoreType.DMA((9,)),
            pltpu.SemaphoreType.DMA((7,)),
            pltpu.SemaphoreType.DMA((7,)),
        ],
        compiler_params=pltpu.CompilerParams(
            collective_id=0, has_side_effects=True, vmem_limit_bytes=56 * 1024 * 1024
        ),
        cost_estimate=pl.CostEstimate(flops=10**9, bytes_accessed=8 * 10**6, transcendentals=10**6),
    )(spectral_coeffs, fields, zonal, fwd, inv, gather, scatter, mlp_in, mlp_mid, mlp_out)


def solution(mesh):
    in_specs = (P(None, "lev", "lon", "lat"), P(None, "lev"), P(), P(), P())
    out_specs = P(None, "lev", "lon", "lat")
    return jax.shard_map(per_device, mesh=mesh, in_specs=in_specs, out_specs=out_specs, check_vma=False)
```

```python
import math

import jax
import jax.numpy as jnp
from jax import lax
from jax.experimental import pallas as pl
from jax.experimental.pallas import tpu as pltpu
from jax.sharding import PartitionSpec as P

WAVES = 320
KMAX = 320
SUBSTEPS = 2
NLON = 960
NLAT = 512
LEVELS = 8
UNITS = 384
GROUP = 64
F32 = jnp.float32
BF16 = jnp.bfloat16


SINE = [(-1.0) ** n * math.pi ** (2 * n + 1) / math.factorial(2 * n + 1) for n in range(7)]


def cosine(half_turns):
    t = jnp.abs(half_turns - 1.0) - 0.5
    square = t * t
    value = jnp.full(t.shape, SINE[-1], F32)
    for term in SINE[-2::-1]:
        value = value * square + term
    return value * t


def split(value):
    high = value.astype(BF16)
    return high, (value - high.astype(F32)).astype(BF16)


def mm(a, b):
    return lax.dot_general(a, b, (((1,), (0,)), ((), ())), preferred_element_type=F32)


def mm_nt(a, b):
    return lax.dot_general(a, b, (((1,), (1,)), ((), ())), preferred_element_type=F32)


def silu(v):
    return 0.5 * v * (1.0 + jnp.tanh(0.5 * v))


def kernel(
    coef_ref, fields_hbm, w_in_hbm, w_mid_hbm, w_out_hbm,
    out_ref,
    fields, zonal, fwd, inv, gather, scatter, w_turned, w_in, w_mid, w_out,
    stage, at, ra, state, vb, ub, mult, mb, rm, cr, fb, ob,
    load_sems, send_sems, recv_sems,
):
    zc = lax.axis_index("lon")
    y = lax.axis_index("lat")
    x = lax.axis_index("lev")
    z, c = lax.div(zc, 2), lax.rem(zc, 2)
    p, zb = lax.div(z, 2), lax.rem(z, 2)
    mine = x * 4 + zb * 2 + c
    me = y * 16 + mine
    own_x, own_b = lax.rem(p, 4), lax.div(p, 4)

    loads = []

    def load(n, src, dst):
        copy = pltpu.make_async_copy(src, dst, load_sems.at[n])
        copy.start()
        loads.append(copy)

    load(0, fields_hbm, fields)
    load(1, w_in_hbm, w_turned)
    load(2, w_mid_hbm, w_mid)
    load(3, w_out_hbm, w_out)

    def group_device(g):
        return {"lon": 4 * p + lax.rem(g, 4), "lat": lax.div(g, 16), "lev": lax.div(lax.rem(g, 16), 4)}

    def first_target(t):
        b, k = lax.div(t, 16), lax.rem(t, 16)
        return {"lon": 4 * (x + 4 * b) + lax.rem(k, 4), "lat": y, "lev": lax.div(k, 4)}

    own_first = x == own_x
    self_t = own_b * 16 + mine

    barrier = pltpu.get_barrier_semaphore()

    def greet_first(j, carry):
        d = lax.rem(zc + j, 32)

        @pl.when(jnp.logical_or(d != zc, jnp.logical_not(own_first)))
        def _():
            pl.semaphore_signal(barrier, inc=1, device_id={"lon": d, "lat": y, "lev": own_x})
        return carry

    def greet_group(j, carry):
        pl.semaphore_signal(barrier, inc=1, device_id=group_device(lax.rem(me + j, GROUP)))
        return carry

    def greet_planes(j, carry):
        pl.semaphore_signal(barrier, inc=1, device_id={"lon": 2 * lax.rem(z + j, 16) + c, "lat": y, "lev": x})
        return carry

    lax.fori_loop(0, 32, greet_first, 0)
    lax.fori_loop(1, GROUP, greet_group, 0)
    lax.fori_loop(1, 16, greet_planes, 0)

    loads[0].wait()
    for b in range(2):
        for f in range(3):
            stage[32 * f : 32 * f + 30, :] = fields[f, :, b, :]
            stage[32 * f + 30 : 32 * f + 32, :] = jnp.zeros((2, 128), F32)
        for n in range(3):
            stage[96 + n : 97 + n, :] = jnp.full((1, 128), coef_ref[b, n], F32)
        stage[99:128, :] = jnp.zeros((29, 128), F32)
        at[128 * b : 128 * b + 128, :] = stage[...].T

    def zonal_block(n, carry):
        turn, v = lax.div(n, 8), lax.rem(n, 8)
        owner = lax.broadcasted_iota(jnp.int32, (GROUP, 128), 0)
        place = lax.broadcasted_iota(jnp.int32, (GROUP, 128), 1)
        wave = 2 * (5 * lax.shift_right_logical(owner, 1) + turn) + (owner & 1)
        r = place & 31
        lon = 30 * (4 * v + lax.shift_right_logical(place, 5)) + r
        product = (wave * lon).astype(F32)
        turns = product - NLON * jnp.floor(product * (1.0 / NLON))
        quarter = jnp.where(turns >= 0.75 * NLON, turns - 0.75 * NLON, turns + 0.25 * NLON)
        for row, steps in ((turn, turns), (5 + turn, quarter)):
            value = jnp.where(r < 30, cosine(steps * (2.0 / NLON)), 0.0)
            high, low = split(value)
            rows = pl.ds(pl.multiple_of(GROUP * row, GROUP), GROUP)
            lanes = pl.ds(pl.multiple_of(128 * v, 128), 128)
            zonal[0, rows, lanes] = high
            zonal[1, rows, lanes] = low
        return carry

    def latitude(deg, place):
        odd = 2 * (8 * (place & 63) + lax.shift_right_logical(place, 6)) + 1
        steps = ((deg + c) * odd - 512 * c) & (4 * NLAT - 1)
        return split(cosine(steps.astype(F32) * (1.0 / (2 * NLAT))))

    def fwd_block(n, carry):
        rows = pl.ds(pl.multiple_of(32 * n, 32), 32)
        deg = 32 * n + lax.broadcasted_iota(jnp.int32, (32, NLAT), 0)
        high, low = latitude(deg, lax.broadcasted_iota(jnp.int32, (32, NLAT), 1))
        fwd[0, rows, :] = high
        fwd[1, rows, :] = low
        return carry

    def inv_block(n, carry):
        rows = pl.ds(pl.multiple_of(32 * n, 32), 32)
        place = 32 * n + lax.broadcasted_iota(jnp.int32, (32, KMAX), 0)
        high, low = latitude(lax.broadcasted_iota(jnp.int32, (32, KMAX), 1), place)
        inv[0, rows, :] = high
        inv[1, rows, :] = low
        return carry

    def lane_tables():
        row = lax.broadcasted_iota(jnp.int32, (24, 256), 0)
        place = lax.broadcasted_iota(jnp.int32, (24, 256), 1)
        base = (row & 7) * 32 + lax.shift_right_logical(row, 3) * 10
        for q in range(10):
            hit = jnp.where(place == base + q, 1.0, 0.0)
            gather[48 * q : 48 * q + 48, :] = jnp.concatenate([hit, hit], axis=0).astype(BF16)
            scatter[24 * q : 24 * q + 24, :] = hit

    lax.fori_loop(0, 40, zonal_block, 0)
    lane_tables()

    pl.semaphore_wait(barrier, 31 + jnp.where(own_first, 0, 1) + (GROUP - 1) + 15)

    def send_first(j, carry):
        t = lax.rem(self_t + j, 32)

        @pl.when(jnp.logical_or(j > 0, jnp.logical_not(own_first)))
        def _():
            pltpu.make_async_remote_copy(
                at.at[pl.ds(pl.multiple_of(8 * t, 8), 8), :],
                ra.at[pl.ds(pl.multiple_of(8 * zc, 8), 8), :],
                send_sems.at[0], recv_sems.at[0], device_id=first_target(t),
            ).start()
        return carry

    lax.fori_loop(0, 32, send_first, 0)

    @pl.when(own_first)
    def _():
        ra[pl.ds(pl.multiple_of(8 * zc, 8), 8), :] = at[pl.ds(pl.multiple_of(8 * self_t, 8), 8), :]

    def drain(ref, sem):
        pltpu.make_async_copy(ref, ref, sem).wait()

    lax.fori_loop(0, 10, fwd_block, 0)
    lax.fori_loop(0, 16, inv_block, 0)
    for n in range(1, 4):
        loads[n].wait()
    w_in[...] = w_turned[...].astype(F32).T.astype(BF16)

    @pl.when(own_first)
    def _():
        drain(ra.at[pl.ds(0, 248), :], recv_sems.at[0])

    @pl.when(jnp.logical_not(own_first))
    def _():
        drain(ra, recv_sems.at[0])

    lane = lax.broadcasted_iota(jnp.int32, (8, 128), 1)
    for v in range(8):
        tiles = [ra[8 * (4 * v + n) : 8 * (4 * v + n) + 8, :] for n in range(4)]
        for f in range(3):
            value = pltpu.roll(tiles[0], (-32 * f) % 128, 1)
            for n in range(1, 4):
                value = jnp.where(lane >= 32 * n, pltpu.roll(tiles[n], (32 * (n - f)) % 128, 1), value)
            state[8 * f : 8 * f + 8, 128 * v : 128 * v + 128] = value

    coefs = ra[0:1, :]

    def operator_tables():
        nu, ga, gb = coefs[:, 96:97], coefs[:, 97:98], coefs[:, 98:99]
        deg = lax.broadcasted_iota(jnp.int32, (KMAX, 32), 0)
        col = lax.broadcasted_iota(jnp.int32, (KMAX, 32), 1)
        field = jnp.where(col >= 20, 2, jnp.where(col >= 10, 1, 0))
        place = col - 10 * field
        turn = jnp.where(place >= 5, place - 5, place)
        wave = 2 * (5 * lax.div(me, 2) + turn) + c
        freq = (deg + c).astype(F32)
        wavef = wave.astype(F32)
        qv = (wavef * wavef + freq * freq) / (KMAX * KMAX)
        scale = jnp.where(wave == 0, 1.0, 2.0) * (2.0 / NLAT / NLON)
        damp = nu * qv * qv
        couple = ga * gb * qv
        den = 1.0 + jnp.where(field == 0, damp, couple)
        own = -jnp.where(field == 0, damp, couple)
        other = jnp.where(field == 0, 0.0, jnp.where(field == 1, ga * qv, -gb))
        valid = col < 30
        factor = jnp.where(valid, scale / den, 0.0)
        mult[0] = own * factor
        mult[1] = other * factor

    for step in range(SUBSTEPS):
        b_in, c_in = 2 * step, 2 * step + 1

        high, low = split(state[...])
        both = jnp.concatenate([high.astype(F32), low.astype(F32)], axis=0).astype(BF16)
        first = jnp.concatenate([high.astype(F32), jnp.zeros((24, 1024), F32)], axis=0).astype(BF16)
        value = mm_nt(zonal[0], both) + mm_nt(zonal[1], first)
        w_high, w_low = split(value)
        packed = jnp.zeros((GROUP, 256), F32)
        for q in range(10):
            rows = slice(GROUP * q, GROUP * q + GROUP)
            place = gather[48 * q : 48 * q + 48, :]
            packed = packed + mm(w_high[rows], place) + mm(w_low[rows], place)

        def exchange(n, value):
            vb[n, pl.ds(0, GROUP, stride=2), :] = value[:, :128]
            vb[n, pl.ds(1, GROUP, stride=2), :] = value[:, 128:]

            def send(j, carry):
                g = lax.rem(me + j, GROUP)
                pltpu.make_async_remote_copy(
                    vb.at[n, pl.ds(2 * g, 2), :], ub.at[n, pl.ds(2 * me, 2), :],
                    send_sems.at[1 + n], recv_sems.at[1 + n], device_id=group_device(g),
                ).start()
                return carry

            lax.fori_loop(1, GROUP, send, 0, unroll=True)
            ub[n, pl.ds(2 * me, 2), :] = vb[n, pl.ds(2 * me, 2), :]

        def received(n):
            drain(ub.at[n, pl.ds(0, 2 * GROUP - 2), :], recv_sems.at[1 + n])
            return jnp.concatenate(
                [ub[n, pl.ds(0, GROUP, stride=2), :], ub[n, pl.ds(1, GROUP, stride=2), :]], axis=1
            )

        exchange(b_in, packed)
        if step == 0:
            operator_tables()
        value = received(b_in)

        value = jnp.concatenate([value[:, 32 * n : 32 * n + 32] for n in range(8)], axis=0)
        high, low = split(value)
        spectra = mm(fwd[0], high) + mm(fwd[0], low) + mm(fwd[1], high)
        col = lax.broadcasted_iota(jnp.int32, (KMAX, 32), 1)
        up = jnp.concatenate([spectra[:, 10:], spectra[:, :10]], axis=1)
        down = jnp.concatenate([spectra[:, 22:], spectra[:, :22]], axis=1)
        change = spectra * mult[0] + jnp.where(col < 20, up, down) * mult[1]
        high, low = split(change)
        value = mm(inv[0], high) + mm(inv[0], low) + mm(inv[1], high)
        value = jnp.concatenate([value[64 * n : 64 * n + 64] for n in range(8)], axis=1)

        exchange(c_in, value)
        value = received(c_in)

        high, low = split(value)
        y_high = mm_nt(scatter[...].astype(BF16), high)
        y_low = mm_nt(scatter[...].astype(BF16), low)
        y_high = jnp.concatenate([y_high[24 * q : 24 * q + 24] for q in range(10)], axis=1)
        y_low = jnp.concatenate([y_low[24 * q : 24 * q + 24] for q in range(10)], axis=1)
        both = jnp.concatenate([y_high, y_low], axis=0).astype(BF16)
        value = mm(both, zonal[0])
        new = state[...] + value[:24] + value[24:] + mm(y_high.astype(BF16), zonal[1])
        state[0:16, :] = new[0:16]
        state[16:24, :] = new[16:24] + 0.25 * new[0:8] * new[8:16]

    half = lane < 64
    for t in range(16):
        v = t // 2
        s = [state[8 * f : 8 * f + 8, 128 * v : 128 * v + 128] for f in range(3)]
        if t % 2 == 0:
            mb[16 * t : 16 * t + 8, :] = jnp.where(half, s[0], pltpu.roll(s[1], 64, 1))
            mb[16 * t + 8 : 16 * t + 16, :] = s[2]
        else:
            mb[16 * t : 16 * t + 8, :] = jnp.where(half, pltpu.roll(s[0], 64, 1), s[1])
            mb[16 * t + 8 : 16 * t + 16, :] = pltpu.roll(s[2], 64, 1)
    slot = zb * 8 + 2 * own_x + own_b

    def send_planes(j, carry):
        t = lax.rem(z + j, 16)
        pltpu.make_async_remote_copy(
            mb.at[pl.ds(pl.multiple_of(16 * t, 16), 16), :], rm.at[pl.ds(pl.multiple_of(16 * slot, 16), 16), :],
            send_sems.at[5], recv_sems.at[5], device_id={"lon": 2 * t + c, "lat": y, "lev": x},
        ).start()
        return carry

    lax.fori_loop(1, 16, send_planes, 0)
    rm[pl.ds(pl.multiple_of(16 * slot, 16), 16), :] = mb[pl.ds(pl.multiple_of(16 * z, 16), 16), :]
    drain(rm.at[pl.ds(0, 240), :], recv_sems.at[5])

    for block in range(4):
        parts = []
        for i8 in (2 * block, 2 * block + 1):
            t00 = rm[pl.ds(i8, 8, stride=16), :]
            t01 = rm[pl.ds(8 + i8, 8, stride=16), :]
            t10 = rm[pl.ds(128 + i8, 8, stride=16), :]
            t11 = rm[pl.ds(128 + 8 + i8, 8, stride=16), :]
            parts.append(jnp.concatenate([
                jnp.where(half, t00, pltpu.roll(t10, 64, 1)),
                jnp.where(half, pltpu.roll(t00, 64, 1), t10),
                jnp.where(half, t01, pltpu.roll(t11, 64, 1)),
            ], axis=0))
        inputs = jnp.concatenate(parts, axis=1).astype(BF16)
        hidden = silu(mm(w_in[...], inputs)).astype(BF16)
        hidden = silu(mm(w_mid[0], hidden)).astype(BF16)
        hidden = silu(mm(w_mid[1], hidden)).astype(BF16)
        result = mm(w_out[...], hidden).astype(BF16).astype(F32)
        for n in range(2):
            for f in range(3):
                row = (f * 8 + 2 * block + n) * 8
                cr[row : row + 8, :] = result[8 * f : 8 * f + 8, 128 * n : 128 * n + 128]

    for l in range(LEVELS):
        t00 = rm[16 * l : 16 * l + 8, :]
        t01 = rm[16 * l + 8 : 16 * l + 16, :]
        t10 = rm[128 + 16 * l : 128 + 16 * l + 8, :]
        t11 = rm[128 + 16 * l + 8 : 128 + 16 * l + 16, :]
        s = [
            jnp.where(half, t00, pltpu.roll(t10, 64, 1)),
            jnp.where(half, pltpu.roll(t00, 64, 1), t10),
            jnp.where(half, t01, pltpu.roll(t11, 64, 1)),
        ]
        s = [s[f] + cr[pl.ds(64 * f + l, 8, stride=8), :] for f in range(3)]
        for bit in range(2):
            for core in range(2):
                n = 2 * bit + core
                value = pltpu.roll(s[0], (-32 * n) % 128, 1)
                for f in range(1, 3):
                    value = jnp.where(lane >= 32 * f, pltpu.roll(s[f], (32 * (f - n)) % 128, 1), value)
                row = (2 * (l // 2) + core) * 32 + (2 * (l % 2) + bit) * 8
                fb[row : row + 8, :] = value

    place = 2 * x + c

    def send_levels(j, carry):
        t = lax.rem(place + j, 8)
        pltpu.make_async_remote_copy(
            fb.at[pl.ds(pl.multiple_of(32 * t, 32), 32), :], ob.at[pl.ds(pl.multiple_of(32 * place, 32), 32), :],
            send_sems.at[6], recv_sems.at[6],
            device_id={"lon": 2 * z + lax.rem(t, 2), "lat": y, "lev": lax.div(t, 2)},
        ).start()
        return carry

    lax.fori_loop(1, 8, send_levels, 0)
    ob[pl.ds(pl.multiple_of(32 * place, 32), 32), :] = fb[pl.ds(pl.multiple_of(32 * place, 32), 32), :]
    drain(ob.at[pl.ds(0, 224), :], recv_sems.at[6])
    for b in range(2):
        rows = []
        for k in range(16):
            row = (2 * (k // 4) + k % 2) * 32 + (2 * b + (k // 2) % 2) * 8
            rows.append(ob[row : row + 8, :])
        stage[...] = jnp.concatenate(rows, axis=0).T
        for f in range(3):
            out_ref[f, :, b, :] = stage[32 * f : 32 * f + 30, :]

    @pl.when(own_first)
    def _():
        drain(at.at[pl.ds(0, 248), :], send_sems.at[0])

    @pl.when(jnp.logical_not(own_first))
    def _():
        drain(at, send_sems.at[0])

    for n in range(4):
        drain(vb.at[n, pl.ds(0, 2 * GROUP - 2), :], send_sems.at[1 + n])
    drain(mb.at[pl.ds(0, 240), :], send_sems.at[5])
    drain(fb.at[pl.ds(0, 224), :], send_sems.at[6])


def per_device(fields, spectral_coeffs, mlp_in, mlp_mid, mlp_out):
    anywhere = pl.BlockSpec(memory_space=pl.ANY)
    vmem = lambda *shape: pltpu.VMEM(shape, F32)
    half = lambda *shape: pltpu.VMEM(shape, BF16)
    fields = fields.transpose(0, 2, 1, 3)
    updated = pl.pallas_call(
        kernel,
        out_shape=jax.ShapeDtypeStruct(fields.shape, F32),
        in_specs=[pl.BlockSpec(memory_space=pltpu.SMEM)] + [anywhere] * 4,
        out_specs=pl.BlockSpec(memory_space=pltpu.VMEM),
        scratch_shapes=[
            vmem(*fields.shape),
            half(2, 2 * WAVES, 1024),
            half(2, KMAX, NLAT),
            half(2, NLAT, KMAX),
            half(480, 256),
            vmem(240, 256),
            half(3 * LEVELS, UNITS),
            half(UNITS, 3 * LEVELS),
            half(2, UNITS, UNITS),
            half(3 * LEVELS, UNITS),
            vmem(128, 128),
            vmem(256, 128),
            vmem(256, 128),
            vmem(24, 1024),
            vmem(4, 128, 128),
            vmem(4, 128, 128),
            vmem(2, KMAX, 32),
            vmem(256, 128),
            vmem(256, 128),
            vmem(192, 128),
            vmem(256, 128),
            vmem(256, 128),
            pltpu.SemaphoreType.DMA((4,)),
            pltpu.SemaphoreType.DMA((7,)),
            pltpu.SemaphoreType.DMA((7,)),
        ],
        compiler_params=pltpu.CompilerParams(
            collective_id=0, has_side_effects=True, vmem_limit_bytes=56 * 1024 * 1024
        ),
        cost_estimate=pl.CostEstimate(flops=10**9, bytes_accessed=8 * 10**6, transcendentals=10**6),
    )(spectral_coeffs.T, fields, mlp_in.T, mlp_mid, mlp_out)
    return updated.transpose(0, 2, 1, 3)


def solution(mesh):
    in_specs = (P(None, "lev", "lon", "lat"), P(None, "lev"), P(), P(), P())
    out_specs = P(None, "lev", "lon", "lat")
    return jax.shard_map(per_device, mesh=mesh, in_specs=in_specs, out_specs=out_specs, check_vma=False)
```
